32 devices in a mesh: rep: 2 (over z, core), dp: 16 (over x, y).
Axes of the slice: x: 4, y: 4, z: 1, core: 2. Of those that a mesh axis runs over, the one named last changes fastest.
The devices are a block of a 4x4x8 slice.
Arguments:
- x: bfloat16 [32, 2048, 1024], P(('rep', 'dp')), parts along dimension 0
- dy: bfloat16 [32, 2048, 1024], P(('rep', 'dp')), parts along dimension 0
- w_gate: bfloat16 [2, 1024, 4096], replicated
- w_up: bfloat16 [2, 1024, 4096], replicated
- w_down: bfloat16 [2, 4096, 1024], replicated
- m_w_gate: float32 [2, 1024, 4096], P(None, 'dp')
- m_w_up: float32 [2, 1024, 4096], P(None, 'dp')
- m_w_down: float32 [2, 4096, 1024], P(None, 'dp')
- v_w_gate: float32 [2, 1024, 4096], P(None, 'dp')
- v_w_up: float32 [2, 1024, 4096], P(None, 'dp')
- v_w_down: float32 [2, 4096, 1024], P(None, 'dp')
Outputs:
- output 1: bfloat16 [4, 1024, 4096], P('rep'), parts along dimension 0
- output 2: bfloat16 [4, 1024, 4096], P('rep'), parts along dimension 0
- output 3: bfloat16 [4, 4096, 1024], P('rep'), parts along dimension 0
- output 4: float32 [4, 1024, 4096], P('rep', 'dp'), parts along dimension 0
- output 5: float32 [4, 1024, 4096], P('rep', 'dp'), parts along dimension 0
- output 6: float32 [4, 4096, 1024], P('rep', 'dp'), parts along dimension 0
- output 7: float32 [4, 1024, 4096], P('rep', 'dp'), parts along dimension 0
- output 8: float32 [4, 1024, 4096], P('rep', 'dp'), parts along dimension 0
- output 9: float32 [4, 4096, 1024], P('rep', 'dp'), parts along dimension 0
There are 2 independent parts. The reference program is written for one: setup_inputs(seed, part) draws one part's arguments, and reference() takes and returns one part's arrays. A program takes and returns all parts, laid end to end along the dimension named above; an argument that names none is the same for every part.
All inputs are finite; a program needn't handle non-finite values.
Results may differ from the reference program's by a relative error of at most 0.022.
Values are sent between devices in bfloat16 or wider.
A program may use at most 768 MiB of HBM per device.

```python
import jax
import jax.numpy as jnp
from jax import lax

SEQUENCES = 16
TOKENS = 2048
D = 1024
FF = 4096
LAYERS = 2
NAMES = ("w_gate", "w_up", "w_down")
SHAPES = {"w_gate": (LAYERS, D, FF), "w_up": (LAYERS, D, FF), "w_down": (LAYERS, FF, D)}


def bump(key, n, height):
    away = (jnp.arange(n, dtype=jnp.int32) - jax.random.randint(key, (), 0, n, jnp.int32)) % n
    return jnp.where(away < n // 8, height, 1.0)


def together(key, own, strength):
    shared = jax.random.normal(key, own.shape[1:], jnp.float32)
    return (own + strength * shared) * lax.rsqrt(1 + strength * strength)


def setup_inputs(seed: int = 0, part: int = 0) -> dict:
    kx, kdy, ka, kb, kz, kf, kh, kl, *keys = jax.random.split(jax.random.key(seed), 8 + 3 * len(NAMES))
    kx, kdy, ka, kb = (jax.random.fold_in(k, part) for k in (kx, kdy, ka, kb))
    kw, km, kv = (keys[i::3] for i in range(3))
    shape = (SEQUENCES, TOKENS, D)
    much_x, much_dy = jax.random.uniform(kz, (2,), jnp.float32, 0.0, 1.0)
    loud = 2.0 ** jax.random.uniform(jax.random.fold_in(kz, 1), (), jnp.float32, -1.0, 2.0)
    layers = 2.0 ** jax.random.uniform(kl, (LAYERS, 1, 1), jnp.float32, -1.0, 1.0)
    x = together(ka, jax.random.normal(kx, shape, jnp.float32), much_x) * bump(kf, D, 4.0)
    dy = together(kb, jax.random.normal(kdy, shape, jnp.float32), much_dy)
    drawn = {"x": x.astype(jnp.bfloat16), "dy": (loud * dy * (SEQUENCES * TOKENS) ** -0.5).astype(jnp.bfloat16)}
    for key, name in zip(kw, NAMES, strict=True):
        w = jax.random.normal(key, SHAPES[name], jnp.float32) * SHAPES[name][1] ** -0.5
        drawn[name] = (w * {"w_gate": 1.0, "w_up": bump(kh, FF, 4.0), "w_down": layers}[name]).astype(jnp.bfloat16)
    for key, name in zip(km, NAMES, strict=True):
        drawn[f"m_{name}"] = 0.1 * jax.random.normal(key, SHAPES[name], jnp.float32)
    for key, name in zip(kv, NAMES, strict=True):
        drawn[f"v_{name}"] = jax.random.uniform(key, SHAPES[name], jnp.float32, 0.005, 0.015)
    return drawn


def matmul(a, w):
    return jnp.dot(a, w, preferred_element_type=jnp.float32).astype(jnp.bfloat16)


def normed(h):
    wide = h.astype(jnp.float32)
    scale = lax.rsqrt(jnp.mean(wide**2, -1, keepdims=True) + 1e-6)
    return (wide * scale).astype(jnp.bfloat16)


def layer(h, w):
    a = normed(h)
    gate = jnp.dot(a, w["w_gate"], preferred_element_type=jnp.float32)
    up = jnp.dot(a, w["w_up"], preferred_element_type=jnp.float32)
    return h + matmul((jax.nn.silu(gate) * up).astype(jnp.bfloat16), w["w_down"])


def adamw(w, m, v, g):
    m = 0.9 * m + 0.1 * g
    v = 0.95 * v + 0.05 * g * g
    step = m * lax.rsqrt(v + 1e-8) + 0.1 * w
    return (w - 0.02 * step).astype(jnp.bfloat16), m, v


def clipped(gradients, sum_of_squares, count):
    factor = jnp.minimum(1.0, 0.5 * lax.rsqrt(sum_of_squares / count + 1e-30))
    return [g * factor for g in gradients]


def stack(weights, h):
    return lax.scan(lambda h, w: (layer(h, w), None), h, weights)[0]


def reference(x, dy, w_gate, w_up, w_down, m_w_gate, m_w_up, m_w_down, v_w_gate, v_w_up, v_w_down):
    weights = dict(zip(NAMES, (w_gate, w_up, w_down), strict=True))

    def take(so_far, sequence):
        h, by_y = sequence
        _, back = jax.vjp(lambda w: stack(w, h), weights)
        return jax.tree.map(lambda total, term: total + term.astype(jnp.float32), so_far, back(by_y)[0]), None

    none_yet = {name: jnp.zeros(w.shape, jnp.float32) for name, w in weights.items()}
    by_weights, _ = lax.scan(take, none_yet, (x, dy))
    gradients = [by_weights[name].astype(jnp.bfloat16).astype(jnp.float32) for name in NAMES]
    gradients = clipped(gradients, sum(jnp.sum(g * g) for g in gradients), sum(g.size for g in gradients))
    new = [
        adamw(w.astype(jnp.float32), m, v, g)
        for w, m, v, g in zip((w_gate, w_up, w_down), (m_w_gate, m_w_up, m_w_down), (v_w_gate, v_w_up, v_w_down), gradients, strict=True)
    ]
    return tuple(one[which] for which in range(3) for one in new)
```

```python
import functools
import jax, jax.numpy as jnp
from jax import lax
from jax.experimental import pallas as pl
from jax.experimental.pallas import tpu as pltpu
from jax.sharding import PartitionSpec as P

BF, F32 = jnp.bfloat16, jnp.float32
NT = (((1,), (1,)), ((), ()))
VMEM = pltpu.CompilerParams(vmem_limit_bytes=60 * 2**20)


def cost(flops, nbytes):
    return pl.CostEstimate(flops=flops, bytes_accessed=nbytes, transcendentals=0)


def mm(a, b):
    return jnp.dot(a, b, preferred_element_type=F32)


def mm_nt(a, b):
    return lax.dot_general(a, b, NT, preferred_element_type=F32)


def gate_up(a, wg, wu, layer, t=None, bn=256, bm=512):
    T, D = a.shape
    FF = wg.shape[2]
    n = FF // bn
    tt = T // n

    def body(a_ref, wg_ref, wu_ref, *refs):
        if t is None:
            z_ref, p_ref, q_ref, tt_ref, x_ref = refs

            @pl.when(pl.program_id(0) == 0)
            def _():
                def rows(i, _):
                    r = pl.ds(pl.multiple_of(i * tt, tt), tt)
                    wide, scale = norm_rows(a_ref[r, :])
                    x_ref[r, :] = (wide * scale).astype(BF)
                    return 0

                lax.fori_loop(0, n, rows, 0)

            tt_ref[...] = x_ref[pl.ds(pl.multiple_of(pl.program_id(0) * tt, tt), tt), :].T
        else:
            t_ref, z_ref, p_ref, q_ref, tt_ref = refs
            x_ref = a_ref
            tt_ref[...] = t_ref[...].T
        for i in range(0, T, bm):
            r = pl.ds(i, bm)
            g = mm(x_ref[r, :], wg_ref[0])
            u = mm(x_ref[r, :], wu_ref[0])
            s = jax.nn.sigmoid(g)
            q = g * s
            z_ref[r, :] = (q * u).astype(BF)
            q_ref[r, :] = q
            p_ref[r, :] = u * (s + q * (1 - s))

    tile = pl.BlockSpec((T, bn), lambda j: (0, j))
    w = pl.BlockSpec((1, D, bn), lambda j: (layer, 0, j))
    shape = jax.ShapeDtypeStruct
    return pl.pallas_call(
        body,
        grid=(n,),
        in_specs=[pl.BlockSpec((T, D), lambda j: (0, 0)), w, w] + [pl.BlockSpec((tt, D), lambda j: (j, 0))] * (t is not None),
        out_specs=[tile, tile, tile, pl.BlockSpec((D, tt), lambda j: (0, j))],
        out_shape=[shape((T, FF), BF), shape((T, FF), F32), shape((T, FF), F32), shape((D, T), BF)],
        scratch_shapes=[pltpu.VMEM((T, D), BF)] * (t is None),
        compiler_params=VMEM,
        cost_estimate=cost(4 * T * D * FF, T * FF * 10),
        name="gate_up",
    )(a, wg, wu, *([] if t is None else [t]))


def norm_rows(h):
    wide = h.astype(F32)
    scale = lax.rsqrt(jnp.mean(wide**2, -1, keepdims=True) + 1e-6)
    return wide, scale


def down(h, z, wd, layer, bm=256):
    T, FF = z.shape
    D = wd.shape[2]

    def body(h_ref, z_ref, w_ref, o_ref, a_ref, at_ref):
        new = h_ref[...] + mm(z_ref[...], w_ref[0]).astype(BF)
        o_ref[...] = new
        wide, scale = norm_rows(new)
        a = (wide * scale).astype(BF)
        a_ref[...] = a
        at_ref[...] = a.T

    row = pl.BlockSpec((bm, D), lambda i: (i, 0))
    return pl.pallas_call(
        body,
        grid=(T // bm,),
        in_specs=[row, pl.BlockSpec((bm, FF), lambda i: (i, 0)), pl.BlockSpec((1, FF, D), lambda i: (layer, 0, 0))],
        out_specs=[row, row, pl.BlockSpec((D, bm), lambda i: (0, i))],
        out_shape=[jax.ShapeDtypeStruct((T, D), BF)] * 2 + [jax.ShapeDtypeStruct((D, T), BF)],
        compiler_params=VMEM,
        cost_estimate=cost(2 * T * D * FF, T * FF * 2 + D * FF * 2),
        name="down",
    )(h, z, wd)


def norm_back(h, da, D):
    wide, scale = norm_rows(h)
    dscale = jnp.sum(da * wide, -1, keepdims=True)
    return (da * scale - wide * (dscale * scale * scale * scale / D)).astype(BF)


PARTS = 4


def swap_even(c, side):
    return c + 1 - 2 * (c % 2)


def swap_odd(c, side):
    return (c + 2 * (c % 2) - 1 + side) % side


def partner(d, part, step, side):
    x, y = d // side, d % side
    swap = swap_even if (part + step) % 2 == 0 else swap_odd
    along_x = (part < 2) == (step < 2)
    return swap(x, side) * side + y if along_x else x * side + swap(y, side)


def new_moments(m, v, g):
    return 0.9 * m + 0.1 * g, 0.95 * v + 0.05 * g * g


def adamw(w, m, v, g):
    m, v = new_moments(m, v, g)
    step = m * lax.rsqrt(v + 1e-8) + 0.1 * w
    return (w - 0.02 * step).astype(BF)


def clip_factor(sum_of_squares, count):
    return jnp.minimum(1.0, 0.5 * lax.rsqrt(sum_of_squares / count + 1e-30))


def new_weights(me, squares, count, gd, gu, ws, ms, vs):
    L, db, FF = ms[0].shape
    fb, D = ms[2].shape[1:]
    H, q, r = gu.shape[1], db // PARTS, fb // PARTS
    h, lane = L * q, 128

    def body(me_ref, sq_ref, gd_ref, gg_ref, gp_ref, *refs):
        (wg, wu, wd), (mg, mu, md), (vg, vu, vd), outs = refs[:3], refs[3:6], refs[6:9], refs[9:-2]
        o_v, g_v = refs[-2:]
        total = jnp.sum(jnp.sum(sq_ref[...], 0, keepdims=True), 1, keepdims=True)
        factor = clip_factor(total, count)

        p = pl.program_id(0)
        for i, (w, m, v, g) in enumerate(((wg, mg, vg, gg_ref), (wu, mu, vu, gp_ref))):
            for l in range(L):
                at = i * h + l * q

                def some(t, _):
                    cols = pl.ds(pl.multiple_of(t * D, D), D)
                    o_v[at : at + q, cols] = adamw(w[l, :, cols].astype(F32), m[l, :, cols], v[l, :, cols], g[l, :, cols].astype(F32) * factor)
                    return 0

                lax.fori_loop(0, FF // D, some, 0)
        first, skip = pl.multiple_of(p * r // lane * lane, lane), pl.multiple_of(p * r % lane, r)
        for l in range(L):
            for t in range(D // H):
                g_v[:, t * H : (t + 1) * H] = gd_ref[l, :, pl.ds(t * fb + first, lane)].astype(F32).T
            new = adamw(wd[l].astype(F32), md[l], vd[l], g_v[pl.ds(skip, r), :] * factor)
            for s in range(0, r, h):
                c = (l * r + s) // h
                o_v[2 * h :, c * D : (c + 1) * D] = new[s : s + h]
        for i, o_ref in enumerate(outs):

            @pl.when(p == i)
            def _(o_ref=o_ref):
                o_ref[...] = o_v[...]

    wide = lambda shape, at: pl.BlockSpec(shape, lambda p, me_ref: (0, at(p, me_ref[0]), 0))
    here, mine = lambda p, me: p, lambda p, me: me * PARTS + p
    row, drow = (L, q, FF), (L, r, D)
    fixed = lambda p, me_ref: (0, 0)
    return pl.pallas_call(
        body,
        grid_spec=pltpu.PrefetchScalarGridSpec(
            num_scalar_prefetch=1,
            grid=(PARTS,),
            in_specs=[pl.BlockSpec(squares.shape, fixed), wide(gd.shape, lambda p, me: 0), wide(row, here), wide(row, lambda p, me: PARTS + p)]
            + [wide(row, mine), wide(row, mine), wide(drow, mine)]
            + [wide(row, here), wide(row, here), wide(drow, here)] * 2,
            out_specs=[pl.BlockSpec((3 * h, FF), fixed)] * PARTS,
            scratch_shapes=[pltpu.VMEM((3 * h, FF), BF), pltpu.VMEM((lane, D), F32)],
        ),
        out_shape=[jax.ShapeDtypeStruct((3 * h, FF), BF)] * PARTS,
        compiler_params=VMEM,
        cost_estimate=cost(10**7, 10**7),
        name="new_weights",
    )(me, squares, gd, gu, gu, *ws, *ms, *vs)


def place(units, owners, parts, shapes, whole):
    (L, db, FF), (_, fb, D), n, axis = shapes
    q, k = db // PARTS, FF // D
    h = L * q
    m = len(units)

    def body(*refs):
        ins, outs, (buf, sin, sout) = refs[:m], refs[-6:-3], refs[-3:]
        me = lax.axis_index(axis)
        gets = [pltpu.make_async_copy(r, buf.at[i], sin.at[i]) for i, r in enumerate(ins)]
        for c in gets:
            c.start()
        puts = []
        for i, (owner, p) in enumerate(zip(owners, parts)):
            gets[i].wait()
            o = owner(me)
            row = pl.multiple_of(o * db + p * q, q)
            here = []
            for w in range(2):
                for l in range(L):
                    here.append((buf.at[i, pl.ds(w * h + l * q, q), :], outs[w].at[l, pl.ds(row, q), :]))
            for c in range(k):
                first = c * h
                l, off = first // (fb // PARTS), first % (fb // PARTS)
                to = pl.multiple_of(o * fb + p * (fb // PARTS) + off, h)
                here.append((buf.at[i, pl.ds(2 * h, h), pl.ds(c * D, D)], outs[2].at[l, pl.ds(to, h), :]))
            for j, (s, t) in enumerate(here):
                c = pltpu.make_async_copy(s, t, sout.at[i, j])
                c.start()
                puts.append(c)
        for c in puts:
            c.wait()

    anys = pl.BlockSpec(memory_space=pl.ANY)
    given = list(units) + (list(whole) if whole is not None else [])
    return pl.pallas_call(
        body,
        in_specs=[anys] * len(given),
        out_specs=[anys] * 3,
        out_shape=[jax.ShapeDtypeStruct((L, n * db, FF), BF)] * 2 + [jax.ShapeDtypeStruct((L, n * fb, D), BF)],
        input_output_aliases={} if whole is None else {m + i: i for i in range(3)},
        scratch_shapes=[pltpu.VMEM((m, 3 * h, FF), BF), pltpu.SemaphoreType.DMA((m,)), pltpu.SemaphoreType.DMA((m, 2 * L + k))],
        cost_estimate=cost(10**8, m * 6 * h * FF * 2),
        name="place",
    )(*given)


def gather(packed, gate, down, axis, n, given, between):
    side = round(n**0.5)
    shapes = (gate, down, n, axis)
    units = [[(packed[p], lambda d: d)] for p in range(PARTS)]
    whole = place([u[0][0] for u in units], [u[0][1] for u in units], range(PARTS), shapes, None)
    sends = []
    for step in (3, 2, 1, 0):
        held = 2 ** (3 - step)
        sends += [(step, i) for i in range(held)]
    rounds = []
    for r, (step, i) in enumerate(sends):
        give = [units[p][i][0] for p in range(PARTS)]
        if r >= 2:
            give, rounds[r - 2] = lax.optimization_barrier((give, rounds[r - 2]))
            for p in range(PARTS):
                units[p][r - 1] = (rounds[r - 2][p], units[p][r - 1][1])
        if r >= 3:
            give, whole = lax.optimization_barrier((give, whole))
        if r == 4:
            give, given = lax.optimization_barrier((give, given))
            done = between(*given)
        if r == 8:
            give, done = lax.optimization_barrier((give, done))
        got = []
        for p in range(PARTS):
            pairs = [(d, partner(d, p, step, side)) for d in range(n)]
            got.append(lax.ppermute(give[p], axis, pairs))
            was = units[p][i][1]
            units[p].append((got[p], lambda d, p=p, step=step, was=was: was(partner(d, p, step, side))))
        rounds.append(got)
        if r >= 2:
            whole = place(rounds[r - 2], [units[p][r - 1][1] for p in range(PARTS)], range(PARTS), shapes, whole)
    for r in (len(sends) - 2, len(sends) - 1):
        whole = place(rounds[r], [units[p][r + 1][1] for p in range(PARTS)], range(PARTS), shapes, whole)
    return whole, done


SLOTS = 15
HELD = ((4, 4), (0, 4), (8, 4), (12, 2), (14, 1))


class Group:
    def __init__(self, index, layer, own, got, out, first, width):
        self.index, self.layer, self.first, self.width = index, layer, first, width
        self.own_ref, self.got_ref, self.out_ref = own, got, out
        self.high = out.shape[1] // PARTS

    def rows(self, p):
        return pl.ds(p * self.high, self.high)

    def cols(self):
        return pl.ds(self.first, self.width)

    def own(self, a, b, p):
        return self.own_ref.at[self.layer, a, b, self.rows(p), self.cols()]

    def got(self, p, first, many):
        return self.got_ref.at[self.layer, p, pl.ds(first, many), :, self.cols()]

    def out(self, p):
        return self.out_ref.at[self.layer, self.rows(p), self.cols()]


class Part:
    def __init__(self, red, on_x, order):
        self.side, self.on_x, self.p = red.side, on_x, order if on_x else order + 2
        (self.c, near, self.c_far), (self.e, e_near, self.e_far) = (red.along_x, red.along_y) if on_x else (red.along_y, red.along_x)
        self.c1, self.c2 = near[order], near[1 - order]
        self.e1, self.e2 = e_near[order], e_near[1 - order]
        self.given = (self.c_far, self.c1)

    def device(self, i, j):
        return i * self.side + j if self.on_x else j * self.side + i

    def own(self, group, i, j):
        return group.own(i, j, self.p) if self.on_x else group.own(j, i, self.p)


class Reducer:
    def __init__(self, axis, side, loaded, sums, kept, ss, load_sem, send_sem, recv_sem, keep_sem):
        self.axis, self.side = axis, side
        self.loaded, self.sums, self.kept, self.ss = loaded, sums, kept, ss
        self.load_sem, self.send_sem, self.recv_sem, self.keep_sem = load_sem, send_sem, recv_sem, keep_sem
        self.last, self.fetched, self.started, self.turn = {}, [], [], 0
        me = lax.axis_index(axis)
        self.x, self.y = me // side, me % side
        self.along_x, self.along_y = self.around(self.x), self.around(self.y)
        self.all = [Part(self, on_x, order) for on_x in (True, False) for order in range(2)]

    def around(self, c):
        odd = c % 2
        return c, (c + 1 - 2 * odd, (c + 2 * odd + self.side - 1) % self.side), (c + 2) % self.side

    def parts(self, do):
        for t in self.all:
            do(t)

    def lines(self):
        s = self.side
        return [[(self.x + d) % s * s + self.y for d in range(1, s)], [self.x * s + (self.y + d) % s for d in range(1, s)]]

    def greet(self):
        barrier = pltpu.get_barrier_semaphore()
        peers = sum(self.lines(), [])
        for peer in peers:
            pl.semaphore_signal(barrier, inc=1, device_id={self.axis: peer}, device_id_type=pl.DeviceIdType.MESH)
        pl.semaphore_wait(barrier, len(peers))

    def remote(self, src, dst, g, p, k, to):
        return pltpu.make_async_remote_copy(
            src_ref=src, dst_ref=dst, send_sem=self.send_sem.at[g, p, k], recv_sem=self.recv_sem.at[g, p, k],
            device_id={self.axis: to}, device_id_type=pl.DeviceIdType.MESH,
        )

    def message(self, group, p, k):
        at = group.got(p, *HELD[k])
        return self.remote(at, at, group.index, p, k, 0)

    def send_columns(self, layer, own, got, groups, first, width):
        cols = pl.ds(pl.multiple_of(first, width), width)
        g = groups[0].index
        for group in groups[1:]:
            g = g + jnp.where(first >= group.first, 1, 0)

        def one(t):
            for k, i in enumerate(t.given):
                rows = groups[0].rows(t.p)
                src = own.at[layer, i, :, rows, cols] if t.on_x else own.at[layer, :, i, rows, cols]
                self.remote(src, got.at[layer, t.p, pl.ds(*HELD[k]), :, cols], g, t.p, k, t.device(t.c1, t.e)).start()

        self.parts(one)

    def send_row(self, group, a):
        def one(t):
            for k, want in enumerate(t.given):
                if t.on_x:

                    @pl.when(a == want)
                    def _():
                        row = group.own(want, slice(None), t.p)
                        self.remote(row, group.got(t.p, *HELD[k]), group.index, t.p, k, t.device(t.c1, t.e)).start()

                else:
                    dst = group.got_ref.at[group.layer, t.p, HELD[k][0] + a, :, group.cols()]
                    self.remote(group.own(a, want, t.p), dst, group.index, t.p, k, t.device(t.c1, t.e)).start()

        self.parts(one)

    def loads(self, group, s, turn, t):
        loaded = self.loaded.at[turn, t.p, :, :, pl.ds(0, group.width)]
        own, got = functools.partial(t.own, group), functools.partial(group.got, t.p)
        if s == 0:
            row = (t.c2, slice(None)) if t.on_x else (slice(None), t.c2)
            srcs = [(group.own(*row, t.p), 0, 4), (got(4, 4), 4, 4)]
        elif s == 1:
            srcs = []
            for i, j in enumerate((t.e1, t.e_far)):
                srcs += [(own(t.c, j), 3 * i, 0), (got(j, 1), 3 * i + 1, 1), (got(8 + j, 1), 3 * i + 2, 1)]
        elif s == 2:
            srcs = [(own(t.c, t.e2), 0, 0), (got(t.e2, 1), 1, 1), (got(8 + t.e2, 1), 2, 1), (got(13, 1), 3, 1)]
        else:
            srcs = [(own(t.c, t.e), 0, 0), (got(t.e, 1), 1, 1), (got(8 + t.e, 1), 2, 1), (got(12, 1), 3, 1), (got(14, 1), 4, 1)]
        return [
            pltpu.make_async_copy(src, loaded.at[pl.ds(i, many)] if many else loaded.at[i], self.load_sem.at[turn, t.p, i]) for src, i, many in srcs
        ]

    def fetch(self, group, s):
        turn = self.turn
        self.turn = 1 - turn

        def one(t):
            for k in ((0,), (1, 2), (3,), (4,))[s]:
                self.message(group, t.p, k).wait_recv()
            for c in self.loads(group, s, turn, t):
                c.start()

        self.parts(one)
        self.fetched.append((group, s, turn))

    def add(self):
        if not self.fetched:
            return
        group, s, turn = self.fetched.pop(0)
        loaded, sums, kept, w = self.loaded, self.sums, self.kept, group.width
        many, at, terms, stride = ((4, 1, 2, 4), (2, 3, 3, 1), (1, 0, 4, 1), (1, 0, 5, 1))[s]
        base = (0, 4, 6, 0)[s]
        before = self.last.get(s)

        def one(t):
            for c in self.loads(group, s, turn, t):
                c.wait()
            if s < 3 and before is not None:
                self.message(before, t.p, s + 2).wait_send()

            step = 512

            def unit(u, _):
                i, cols = u // (w // step), pl.ds(pl.multiple_of(u % (w // step) * step, step), step)
                total = sum(loaded[turn, t.p, i * at + m * stride, :, cols].astype(F32) for m in range(terms)).astype(BF)
                if s < 3:
                    sums[t.p, base + i, :, cols] = total
                else:
                    kept[t.p, :, cols] = total
                    sq = total.astype(F32)
                    sq = (sq * sq).reshape(-1, *self.ss.shape[:1], step).sum(0)
                    self.ss[...] += sum(sq[:, m : m + 128] for m in range(0, step, 128))
                return 0

            lax.fori_loop(0, many * (w // step), unit, 0)
            if s < 3:
                to = (t.device(t.c2, t.e), t.device(t.c, t.e1), t.device(t.c, t.e2))[s]
                src = sums.at[t.p, pl.ds(base, HELD[s + 2][1]), :, pl.ds(0, w)]
                self.remote(src, group.got(t.p, *HELD[s + 2]), group.index, t.p, s + 2, to).start()
            else:
                self.keep(group, t.p).start()

        if s == 3 and before is not None:
            self.parts(lambda t: self.keep(before, t.p).wait())
        self.parts(one)
        self.last[s] = group
        if s == 0:
            self.started.append(group)

    def keep(self, group, p):
        return pltpu.make_async_copy(self.kept.at[p, :, pl.ds(0, group.width)], group.out(p), self.keep_sem.at[p])

    def finish(self):
        def one(t):
            for group in self.started:
                for k in (0, 1):
                    self.message(group, t.p, k).wait_send()
            for s in range(3):
                self.message(self.last[s], t.p, s + 2).wait_send()
            self.keep(self.last[3], t.p).wait()

        self.parts(one)

    def total(self, out, got, send_sem, recv_sem):
        src = self.ss
        for k, (place, line) in enumerate(zip((self.x, self.y), self.lines())):
            got[k, place] = src[...]
            copies = [
                pltpu.make_async_remote_copy(
                    src_ref=src, dst_ref=got.at[k, place], send_sem=send_sem.at[k, d], recv_sem=recv_sem.at[k, d],
                    device_id={self.axis: peer}, device_id_type=pl.DeviceIdType.MESH,
                )
                for d, peer in enumerate(line)
            ]
            for c in copies:
                c.start()
            for c in copies:
                c.wait()
            out[...] = sum(got[k, i] for i in range(self.side))
            src = out


def reduce_scratch(high, wide, groups, side):
    dma = pltpu.SemaphoreType.DMA
    vec = (8, 128)
    return [
        pltpu.VMEM((2, PARTS, 8, high, wide), BF), pltpu.VMEM((PARTS, 7, high, wide), BF), pltpu.VMEM((PARTS, high, wide), BF), pltpu.VMEM(vec, F32),
        dma((2, PARTS, 8)), dma((groups, PARTS, 5)), dma((groups, PARTS, 5)), dma((PARTS,)),
        pltpu.VMEM(vec, F32), pltpu.VMEM((2, side, *vec), F32), dma((2, side)), dma((2, side)),
    ]


def pipeline(n, loads, work, stores, ready=(), after=None, every=1, hooks=None):
    for c in loads(0, 0):
        c.start()
    for f in ready:
        f()

    def written(j):
        for c in stores(j, j % 2):
            c.wait()

    def tile(j, _):
        slot = j % 2

        @pl.when(j + 1 < n)
        def _():
            for c in loads(j + 1, 1 - slot):
                c.start()

        for c in loads(j, slot):
            c.wait()
        work(j, slot)
        for c in stores(j, slot):
            c.start()

        @pl.when(j > 0)
        def _():
            written(j - 1)

        if after is not None:

            @pl.when((j > 0) & (j % every == 0))
            def _():
                after(j - every)

        for at, todo in (hooks or {}).items():

            @pl.when(j == at)
            def _(todo=todo):
                for f in todo:
                    f()

        return 0

    lax.fori_loop(0, n, tile, 0)
    written(n - 1)
    if after is not None:
        after(n - every)


def backward(dy, dyt, wg, wu, wd, h1, a0t, a1t, z0, p0, q0, z1, p1, q1, axis, n):
    T, D = dy.shape
    FF = z0.shape[1]
    db, fb, side, L = D // n, FF // n, round(n**0.5), wg.shape[0]
    H = 2 * db
    high, wide = H // PARTS, D // H * fb
    cuts = ((0, FF // 2, FF // 8 * 7, FF), (0, FF // 2, FF))
    bd, bg, bt = 2 * fb, 256, 256
    k = bd // fb
    n_groups = L + sum(len(c) - 1 for c in cuts)
    piece = 512

    def body(dy_h, dyt_h, wg_h, wu_h, wd_h, h1_h, a0t_h, a1t_h, z0_h, p0_h, q0_h, z1_h, p1_h, q1_h, *refs):
        (d_out, gu_out, ss_out, d_got, gu_got, d_own, gu_own, dg_h, du_h) = refs[:9]
        (dy_v, dyt_v, at_v, w_v, res_sem) = refs[9:14]
        red = Reducer(axis, side, *refs[14:-4])
        copy = pltpu.make_async_copy
        count = iter(range(n_groups))
        down_of = [Group(next(count), l, d_own, d_got, d_out, 0, wide) for l in range(L)]
        gate_of = [[Group(next(count), l, gu_own, gu_got, gu_out, a, b - a) for a, b in zip(cuts[l], cuts[l][1:])] for l in range(L)]

        named = dict(zip("dDabcAB", down_of + gate_of[0] + gate_of[1]))
        left = {name: iter(range(4)) for name in named}

        def fetch(name):
            red.fetch(named[name], next(left[name]))

        def steps(plan):
            hooks = {}
            for t, name in enumerate(plan):
                if t and plan[t - 1] != ".":
                    hooks[t] = [red.add]
                if name != ".":
                    hooks.setdefault(t, []).append(functools.partial(fetch, name))
            return hooks

        def down_grad(l, z_h, plan, ready):
            def scope(z_v, o_v, zs, os):
                def loads(j, slot):
                    return [copy(z_h.at[:, pl.ds(pl.multiple_of(j * bd, bd), bd)], z_v.at[slot], zs.at[slot])]

                def stores(j, slot):
                    a, b = j * k // side, j * k % side
                    return [copy(o_v.at[slot], d_own.at[l, a, pl.ds(b, k)], os.at[slot])]

                def work(j, slot):
                    for i in range(D // piece):
                        g = mm(dyt_v[pl.ds(i * piece, piece), :], z_v[slot]).astype(BF)
                        for r in range(piece // H):
                            to = (i * (piece // H) + r) * fb
                            for c in range(k):
                                o_v[slot, c, :, to : to + fb] = g[r * H : (r + 1) * H, c * fb : (c + 1) * fb]

                def after(j):
                    red.send_row(down_of[l], j * k // side)

                pipeline(FF // bd, loads, work, stores, ready, after, side // k, steps(plan))
                red.add()

            two = pltpu.SemaphoreType.DMA((2,))
            pl.run_scoped(scope, pltpu.VMEM((2, T, bd), BF), pltpu.VMEM((2, k, H, wide), BF), two, two)

        def gate_up_grad(l, p_h, q_h, keep, every, plan, ready):
            def scope(w_t, p_v, q_v, dg_v, du_v, o_v, ins, os):
                def tile(j):
                    return pl.ds(pl.multiple_of(j * bg, bg), bg)

                def loads(j, slot):
                    pairs = ((wd_h.at[l, tile(j), :], w_t), (p_h.at[:, tile(j)], p_v), (q_h.at[:, tile(j)], q_v))
                    return [copy(src, dst.at[slot], ins.at[slot, i]) for i, (src, dst) in enumerate(pairs)]

                def stores(j, slot):
                    out = [copy(o_v.at[slot], gu_own.at[l, :, :, :, tile(j)], os.at[slot, 0])]
                    if keep:
                        out.append(copy(dg_v.at[slot], dg_h.at[:, tile(j)], os.at[slot, 1]))
                        out.append(copy(du_v.at[slot], du_h.at[:, tile(j)], os.at[slot, 2]))
                    return out

                def work(j, slot):
                    for i in range(0, T, piece):
                        at = pl.ds(i, piece)
                        dz = mm_nt(dy_v[at, :], w_t[slot]).astype(BF).astype(F32)
                        dg_v[slot, at, :] = (dz * p_v[slot, at, :]).astype(BF)
                        du_v[slot, at, :] = (dz * q_v[slot, at, :]).astype(BF)
                    for i in range(0, D, piece):
                        at = pl.ds(i, piece)
                        for half, d_v in enumerate((dg_v, du_v)):
                            g = mm(at_v[at, :], d_v[slot]).astype(BF)
                            for b in range(piece // db):
                                block = i // db + b
                                o_v[slot, block // side, block % side, half * db : (half + 1) * db, :] = g[b * db : (b + 1) * db]

                def after(j):
                    red.send_columns(l, gu_own, gu_got, gate_of[l], j * bg, every * bg)

                pipeline(FF // bg, loads, work, stores, ready, after, every, steps(plan))
                red.add()

            six = pltpu.SemaphoreType.DMA((2, 3))
            f, b = pltpu.VMEM((2, T, bg), F32), pltpu.VMEM((2, T, bg), BF)
            pl.run_scoped(scope, pltpu.VMEM((2, bg, D), BF), f, f, b, b, pltpu.VMEM((2, side, side, H, bg), BF), six, six)

        def norm_grad(plan, ready):
            def scope(dg_v, du_v, h_v, da_0, da_1, ins):
                def tile(j):
                    return pl.ds(pl.multiple_of(j * bt, bt), bt)

                def rows_before(j):
                    return tile(jnp.maximum(j - 1, 0))

                def loads(j, slot):
                    pairs = ((dg_h.at[tile(j), :], dg_v), (du_h.at[tile(j), :], du_v), (h1_h.at[rows_before(j), :], h_v))
                    return [copy(src, dst.at[slot], ins.at[slot, i]) for i, (src, dst) in enumerate(pairs)]

                def one(j, slot, da_v, before_v):
                    at = rows_before(j)
                    old = dy_v[at, :]
                    new = old + norm_back(h_v[slot], before_v[...].astype(F32), D)
                    new = jnp.where(j > 0, new, old)
                    da_v[...] = mm_nt(dg_v[slot], w_v[0]).astype(BF) + mm_nt(du_v[slot], w_v[1]).astype(BF)
                    dy_v[at, :] = new
                    dyt_v[:, at] = new.T

                def work(j, slot):
                    for s, pair in enumerate(((da_0, da_1), (da_1, da_0))):
                        pl.when(slot == s)(functools.partial(one, j, s, *pair))

                pipeline(T // bt, loads, work, lambda j, slot: [], ready, hooks=steps(plan))
                last = T // bt
                get_h = copy(h1_h.at[rows_before(last), :], h_v.at[last % 2], ins.at[last % 2, 2])
                get_h.start()
                red.add()
                get_h.wait()
                at = rows_before(last)
                new = dy_v[at, :] + norm_back(h_v[last % 2], (da_1 if last % 2 == 0 else da_0)[...].astype(F32), D)
                dy_v[at, :] = new
                dyt_v[:, at] = new.T

            wide_t, da = pltpu.VMEM((2, bt, FF), BF), pltpu.VMEM((bt, D), BF)
            pl.run_scoped(scope, wide_t, wide_t, pltpu.VMEM((2, bt, D), BF), da, da, pltpu.SemaphoreType.DMA((2, 3)))

        def resident(i, src, dst):
            return copy(src, dst, res_sem.at[i])

        get_dyt, get_dy, get_at = resident(0, dyt_h, dyt_v), resident(1, dy_h, dy_v), resident(2, a1t_h, at_v)
        get_wg, get_wu, get_at0 = resident(3, wg_h.at[1], w_v.at[0]), resident(4, wu_h.at[1], w_v.at[1]), resident(5, a0t_h, at_v)
        get_dyt.start()
        red.greet()
        red.ss[...] = jnp.zeros_like(red.ss)
        down_grad(1, z1_h, "", (get_dyt.wait, get_dy.start, get_at.start, get_wg.start, get_wu.start))
        gate_up_grad(1, p1_h, q1_h, True, 4, "......D....D..A.", (get_dy.wait, get_at.wait))
        get_at0.start()
        norm_grad("D.A.B...", (get_wg.wait, get_wu.wait))
        down_grad(0, z0_h, "A..B....", ())
        gate_up_grad(0, p0_h, q0_h, False, 2, "B.d...d.a.......", (get_at0.wait,))
        for name in "AbBcDdabcdabcabc":
            fetch(name)
            red.add()
        red.finish()
        out, *rest = refs[-4:]
        red.total(out, *rest)
        ss_out[...] = out[...]

    anys = pl.BlockSpec(memory_space=pl.ANY)
    shape = jax.ShapeDtypeStruct
    return pl.pallas_call(
        body,
        in_specs=[anys] * 14,
        out_specs=[anys, anys, pl.BlockSpec(memory_space=pltpu.VMEM)] + [anys] * 6,
        out_shape=[
            shape((L, H, wide), BF), shape((L, H, FF), BF), shape((8, 128), F32),
            shape((L, PARTS, SLOTS, high, wide), BF), shape((L, PARTS, SLOTS, high, FF), BF),
            shape((L, side, side, H, wide), BF), shape((L, side, side, H, FF), BF), shape((T, FF), BF), shape((T, FF), BF),
        ],
        scratch_shapes=[pltpu.VMEM((T, D), BF), pltpu.VMEM((D, T), BF), pltpu.VMEM((D, T), BF), pltpu.VMEM((2, D, FF), BF), pltpu.SemaphoreType.DMA((6,))]
        + reduce_scratch(high, wide, n_groups, side),
        compiler_params=pltpu.CompilerParams(collective_id=0, has_side_effects=True, vmem_limit_bytes=67043328),
        cost_estimate=cost(18 * T * D * FF, 10**9),
        name="backward",
    )(dy, dyt, wg, wu, wd, h1, a0t, a1t, z0, p0, q0, z1, p1, q1)[:3]


def solution(mesh):
    axis = "dp"
    n = mesh.shape[axis]

    def step(x, dy, wg, wu, wd, mg, mu, md, vg, vu, vd):
        x, dy = x[0], dy[0]
        z0, p0, q0, a0t = gate_up(x, wg, wu, 0)
        h1, a1, a1t = down(x, z0, wd, 0)
        z1, p1, q1, dyt = gate_up(a1, wg, wu, 1, dy)
        gd, gu, squares = backward(dy, dyt, wg, wu, wd, h1, a0t, a1t, z0, p0, q0, z1, p1, q1, axis, n)

        ws, ms, vs = (wg, wu, wd), (mg, mu, md), (vg, vu, vd)
        count = n * sum(m.size for m in ms)
        me = lax.axis_index(axis).reshape(1)
        packed = new_weights(me, squares, count, gd, gu, ws, ms, vs)

        def moments(gd, gu, squares):
            factor = clip_factor(jnp.sum(squares), count)
            (L, db), fb = mg.shape[:2], md.shape[1]
            by_down = gd.reshape(*gd.shape[:2], -1, fb).transpose(0, 3, 2, 1).reshape(md.shape)
            new = [new_moments(m, v, g.astype(F32) * factor) for m, v, g in zip(ms, vs, (gu[:, :db], gu[:, db:], by_down))]
            return [t[0] for t in new] + [t[1] for t in new]

        whole, done = gather(packed, mg.shape, md.shape, axis, n, (gd, gu, squares), moments)
        return (*whole, *done)

    seq, all_, rows = P(("rep", axis)), P(), P(None, axis)
    return jax.shard_map(
        step,
        mesh=mesh,
        in_specs=(seq, seq, *[all_] * 3, *[rows] * 6),
        out_specs=(*[P("rep")] * 3, *[P("rep", axis)] * 6),
        check_vma=False,
    )
```

```python
import functools
import jax, jax.numpy as jnp
from jax import lax
from jax.experimental import pallas as pl
from jax.experimental.pallas import tpu as pltpu
from jax.sharding import PartitionSpec as P

BF, F32 = jnp.bfloat16, jnp.float32
NT = (((1,), (1,)), ((), ()))
VMEM = pltpu.CompilerParams(vmem_limit_bytes=60 * 2**20)


def cost(flops, nbytes):
    return pl.CostEstimate(flops=flops, bytes_accessed=nbytes, transcendentals=0)


def mm(a, b):
    return jnp.dot(a, b, preferred_element_type=F32)


def mm_nt(a, b):
    return lax.dot_general(a, b, NT, preferred_element_type=F32)


def norm_rows(h):
    wide = h.astype(F32)
    scale = lax.rsqrt(jnp.mean(wide**2, -1, keepdims=True) + 1e-6)
    return wide, scale


def forward(x, dy, wg, wu, wd, bn=256, bm=512, bt=256):
    T, D = x.shape
    L, _, FF = wg.shape
    n, m = FF // bn, T // bt
    tt = T // n

    def body(x_ref, dy_ref, wg_ref, wu_ref, wd_h, z_ref, p_ref, q_ref, h_ref, a0t_ref, a1t_ref, dyt_ref, a_v, z_v, wd_v, sem):
        j = pl.program_id(0)
        get = pltpu.make_async_copy(wd_h.at[0], wd_v, sem)

        @pl.when(j == 0)
        def _():
            get.start()

            def rows(k, _):
                r = pl.ds(pl.multiple_of(k * tt, tt), tt)
                wide, scale = norm_rows(x_ref[r, :])
                a_v[r, :] = (wide * scale).astype(BF)
                return 0

            lax.fori_loop(0, n, rows, 0)

        @pl.when(j < n)
        def _():
            a0t_ref[...] = a_v[pl.ds(pl.multiple_of(j * tt, tt), tt), :].T

        @pl.when(j >= n + m)
        def _():
            dyt_ref[...] = dy_ref[...].T

        @pl.when((j < n) | (j >= n + m))
        def _():
            cols = pl.ds(pl.multiple_of(tile(j) * bn, bn), bn)
            for k in range(0, T, bm):
                r = pl.ds(k, bm)
                g = mm(a_v[r, :], wg_ref[0])
                u = mm(a_v[r, :], wu_ref[0])
                s = jax.nn.sigmoid(g)
                q = g * s
                z = (q * u).astype(BF)
                z_ref[0, r, :] = z
                z_v[r, cols] = z
                q_ref[0, r, :] = q
                p_ref[0, r, :] = u * (s + q * (1 - s))

        @pl.when(j == n)
        def _():
            get.wait()

        @pl.when((j >= n) & (j < n + m))
        def _():
            r = pl.ds(pl.multiple_of((j - n) * bt, bt), bt)
            new = x_ref[r, :] + mm(z_v[r, :], wd_v[...]).astype(BF)
            h_ref[...] = new
            wide, scale = norm_rows(new)
            a = (wide * scale).astype(BF)
            a_v[r, :] = a
            a1t_ref[...] = a.T

    def layer(j):
        return jnp.where(j < n + m, 0, 1)

    def tile(j):
        return jnp.where(j < n + m, jnp.minimum(j, n - 1), j - n - m)

    def row(j):
        return jnp.clip(j - n, 0, m - 1)

    def late(j):
        return jnp.maximum(j - n - m, 0)

    w = pl.BlockSpec((1, D, bn), lambda j: (layer(j), 0, tile(j)))
    o = pl.BlockSpec((1, T, bn), lambda j: (layer(j), 0, tile(j)))
    shape = jax.ShapeDtypeStruct
    return pl.pallas_call(
        body,
        grid=(2 * n + m,),
        in_specs=[pl.BlockSpec((T, D), lambda j: (0, 0)), pl.BlockSpec((tt, D), lambda j: (late(j), 0)), w, w, pl.BlockSpec(memory_space=pl.ANY)],
        out_specs=[
            o, o, o, pl.BlockSpec((bt, D), lambda j: (row(j), 0)), pl.BlockSpec((D, tt), lambda j: (0, jnp.minimum(j, n - 1))),
            pl.BlockSpec((D, bt), lambda j: (0, row(j))), pl.BlockSpec((D, tt), lambda j: (0, late(j))),
        ],
        out_shape=[shape((L, T, FF), BF), shape((L, T, FF), F32), shape((L, T, FF), F32), shape((T, D), BF), *[shape((D, T), BF)] * 3],
        scratch_shapes=[pltpu.VMEM((T, D), BF), pltpu.VMEM((T, FF), BF), pltpu.VMEM((FF, D), BF), pltpu.SemaphoreType.DMA],
        compiler_params=VMEM,
        cost_estimate=cost(10 * T * D * FF, T * FF * 20),
        name="forward",
    )(x, dy, wg, wu, wd)


def norm_back(h, da, D):
    wide, scale = norm_rows(h)
    dscale = jnp.sum(da * wide, -1, keepdims=True)
    return (da * scale - wide * (dscale * scale * scale * scale / D)).astype(BF)


PARTS = 4


def swap_even(c, side):
    return c + 1 - 2 * (c % 2)


def swap_odd(c, side):
    return (c + 2 * (c % 2) - 1 + side) % side


def partner(d, part, step, side):
    x, y = d // side, d % side
    swap = swap_even if (part + step) % 2 == 0 else swap_odd
    along_x = (part < 2) == (step < 2)
    return swap(x, side) * side + y if along_x else x * side + swap(y, side)


def new_moments(m, v, g):
    return 0.9 * m + 0.1 * g, 0.95 * v + 0.05 * g * g


def adamw(w, m, v, g):
    m, v = new_moments(m, v, g)
    step = m * lax.rsqrt(v + 1e-8) + 0.1 * w
    return (w - 0.02 * step).astype(BF)


def clip_factor(sum_of_squares, count):
    return jnp.minimum(1.0, 0.5 * lax.rsqrt(sum_of_squares / count + 1e-30))


def place(units, owners, parts, shapes, whole):
    (L, db, FF), (_, fb, D), n, axis = shapes
    q, k = db // PARTS, FF // D
    h = L * q
    m = len(units)

    def body(*refs):
        ins, outs, (buf, sin, sout) = refs[:m], refs[-6:-3], refs[-3:]
        me = lax.axis_index(axis)
        gets = [pltpu.make_async_copy(r, buf.at[i], sin.at[i]) for i, r in enumerate(ins)]
        for c in gets:
            c.start()
        puts = []
        for i, (owner, p) in enumerate(zip(owners, parts)):
            gets[i].wait()
            o = owner(me)
            row = pl.multiple_of(o * db + p * q, q)
            here = []
            for w in range(2):
                for l in range(L):
                    here.append((buf.at[i, pl.ds(w * h + l * q, q), :], outs[w].at[l, pl.ds(row, q), :]))
            for c in range(k):
                first = c * h
                l, off = first // (fb // PARTS), first % (fb // PARTS)
                to = pl.multiple_of(o * fb + p * (fb // PARTS) + off, h)
                here.append((buf.at[i, pl.ds(2 * h, h), pl.ds(c * D, D)], outs[2].at[l, pl.ds(to, h), :]))
            for j, (s, t) in enumerate(here):
                c = pltpu.make_async_copy(s, t, sout.at[i, j])
                c.start()
                puts.append(c)
        for c in puts:
            c.wait()

    anys = pl.BlockSpec(memory_space=pl.ANY)
    given = list(units) + (list(whole) if whole is not None else [])
    return pl.pallas_call(
        body,
        in_specs=[anys] * len(given),
        out_specs=[anys] * 3,
        out_shape=[jax.ShapeDtypeStruct((L, n * db, FF), BF)] * 2 + [jax.ShapeDtypeStruct((L, n * fb, D), BF)],
        input_output_aliases={} if whole is None else {m + i: i for i in range(3)},
        scratch_shapes=[pltpu.VMEM((m, 3 * h, FF), BF), pltpu.SemaphoreType.DMA((m,)), pltpu.SemaphoreType.DMA((m, 2 * L + k))],
        cost_estimate=cost(10**8, m * 6 * h * FF * 2),
        name="place",
    )(*given)


def gather(packed, gate, down, axis, n, given, between):
    side = round(n**0.5)
    shapes = (gate, down, n, axis)
    units = [[(packed[p], lambda d: d)] for p in range(PARTS)]
    whole = place([u[0][0] for u in units], [u[0][1] for u in units], range(PARTS), shapes, None)
    sends = []
    for step in (3, 2, 1, 0):
        held = 2 ** (3 - step)
        sends += [(step, i) for i in range(held)]
    rounds = []
    for r, (step, i) in enumerate(sends):
        give = [units[p][i][0] for p in range(PARTS)]
        if r >= 2:
            give, rounds[r - 2] = lax.optimization_barrier((give, rounds[r - 2]))
            for p in range(PARTS):
                units[p][r - 1] = (rounds[r - 2][p], units[p][r - 1][1])
        if r >= 3:
            give, whole = lax.optimization_barrier((give, whole))
        if r == 4:
            give, given = lax.optimization_barrier((give, given))
            done = between(*given)
        if r == 8:
            give, done = lax.optimization_barrier((give, done))
        got = []
        for p in range(PARTS):
            pairs = [(d, partner(d, p, step, side)) for d in range(n)]
            got.append(lax.ppermute(give[p], axis, pairs))
            was = units[p][i][1]
            units[p].append((got[p], lambda d, p=p, step=step, was=was: was(partner(d, p, step, side))))
        rounds.append(got)
        if r >= 2:
            whole = place(rounds[r - 2], [units[p][r - 1][1] for p in range(PARTS)], range(PARTS), shapes, whole)
    for r in (len(sends) - 2, len(sends) - 1):
        whole = place(rounds[r], [units[p][r + 1][1] for p in range(PARTS)], range(PARTS), shapes, whole)
    return whole, done


SLOTS = 15
HELD = ((4, 4), (0, 4), (8, 4), (12, 2), (14, 1))


class Group:
    def __init__(self, index, layer, own, got, out, first, width):
        self.index, self.layer, self.first, self.width = index, layer, first, width
        self.own_ref, self.got_ref, self.out_ref = own, got, out
        self.high = out.shape[1] // PARTS

    def rows(self, p):
        return pl.ds(p * self.high, self.high)

    def cols(self):
        return pl.ds(self.first, self.width)

    def own(self, a, b, p):
        return self.own_ref.at[self.layer, a, b, self.rows(p), self.cols()]

    def got(self, p, first, many):
        return self.got_ref.at[self.layer, p, pl.ds(first, many), :, self.cols()]


class Part:
    def __init__(self, red, on_x, order):
        self.side, self.on_x, self.p = red.side, on_x, order if on_x else order + 2
        (self.c, near, self.c_far), (self.e, e_near, self.e_far) = (red.along_x, red.along_y) if on_x else (red.along_y, red.along_x)
        self.c1, self.c2 = near[order], near[1 - order]
        self.e1, self.e2 = e_near[order], e_near[1 - order]
        self.given = (self.c_far, self.c1)

    def device(self, i, j):
        return i * self.side + j if self.on_x else j * self.side + i

    def own(self, group, i, j):
        return group.own(i, j, self.p) if self.on_x else group.own(j, i, self.p)


class Reducer:
    def __init__(self, axis, side, loaded, sums, ss, load_sem, send_sem, recv_sem):
        self.axis, self.side = axis, side
        self.loaded, self.sums, self.ss = loaded, sums, ss
        self.load_sem, self.send_sem, self.recv_sem = load_sem, send_sem, recv_sem
        self.last, self.fetched, self.started = {}, None, []
        me = lax.axis_index(axis)
        self.x, self.y = me // side, me % side
        self.along_x, self.along_y = self.around(self.x), self.around(self.y)
        self.all = [Part(self, on_x, order) for on_x in (True, False) for order in range(2)]

    def around(self, c):
        odd = c % 2
        return c, (c + 1 - 2 * odd, (c + 2 * odd + self.side - 1) % self.side), (c + 2) % self.side

    def parts(self, do):
        for t in self.all:
            do(t)

    def lines(self):
        s = self.side
        return [[(self.x + d) % s * s + self.y for d in range(1, s)], [self.x * s + (self.y + d) % s for d in range(1, s)]]

    def greet(self):
        barrier = pltpu.get_barrier_semaphore()
        peers = sum(self.lines(), [])
        for peer in peers:
            pl.semaphore_signal(barrier, inc=1, device_id={self.axis: peer}, device_id_type=pl.DeviceIdType.MESH)
        pl.semaphore_wait(barrier, len(peers))

    def remote(self, src, dst, g, p, k, to):
        return pltpu.make_async_remote_copy(
            src_ref=src, dst_ref=dst, send_sem=self.send_sem.at[g, p, k], recv_sem=self.recv_sem.at[g, p, k],
            device_id={self.axis: to}, device_id_type=pl.DeviceIdType.MESH,
        )

    def message(self, group, p, k):
        at = group.got(p, *HELD[k])
        return self.remote(at, at, group.index, p, k, 0)

    def send_columns(self, layer, own, got, groups, first, width):
        cols = pl.ds(pl.multiple_of(first, width), width)
        g = groups[0].index
        for group in groups[1:]:
            g = g + jnp.where(first >= group.first, 1, 0)

        def one(t):
            for k, i in enumerate(t.given):
                rows = groups[0].rows(t.p)
                src = own.at[layer, i, :, rows, cols] if t.on_x else own.at[layer, :, i, rows, cols]
                self.remote(src, got.at[layer, t.p, pl.ds(*HELD[k]), :, cols], g, t.p, k, t.device(t.c1, t.e)).start()

        self.parts(one)

    def send_row(self, group, a):
        def one(t):
            for k, want in enumerate(t.given):
                if t.on_x:

                    @pl.when(a == want)
                    def _():
                        row = group.own(want, slice(None), t.p)
                        self.remote(row, group.got(t.p, *HELD[k]), group.index, t.p, k, t.device(t.c1, t.e)).start()

                else:
                    dst = group.got_ref.at[group.layer, t.p, HELD[k][0] + a, :, group.cols()]
                    self.remote(group.own(a, want, t.p), dst, group.index, t.p, k, t.device(t.c1, t.e)).start()

        self.parts(one)

    def loads(self, group, s, t):
        loaded = self.loaded.at[t.p, :, :, pl.ds(0, group.width)]
        own, got = functools.partial(t.own, group), functools.partial(group.got, t.p)
        if s == 0:
            row = (t.c2, slice(None)) if t.on_x else (slice(None), t.c2)
            srcs = [(group.own(*row, t.p), 0, 4), (got(4, 4), 4, 4)]
        elif s == 1:
            srcs = []
            for i, j in enumerate((t.e1, t.e_far)):
                srcs += [(own(t.c, j), 3 * i, 0), (got(j, 1), 3 * i + 1, 1), (got(8 + j, 1), 3 * i + 2, 1)]
        elif s == 2:
            srcs = [(own(t.c, t.e2), 0, 0), (got(t.e2, 1), 1, 1), (got(8 + t.e2, 1), 2, 1), (got(13, 1), 3, 1)]
        else:
            srcs = [(own(t.c, t.e), 0, 0), (got(t.e, 1), 1, 1), (got(8 + t.e, 1), 2, 1), (got(12, 1), 3, 1), (got(14, 1), 4, 1)]
        return [
            pltpu.make_async_copy(src, loaded.at[pl.ds(i, many)] if many else loaded.at[i], self.load_sem.at[t.p, i]) for src, i, many in srcs
        ]

    def fetch(self, group, s):
        def one(t):
            for k in ((0,), (1, 2), (3,), (4,))[s]:
                self.message(group, t.p, k).wait_recv()
            for c in self.loads(group, s, t):
                c.start()

        self.parts(one)
        self.fetched = group, s

    def add(self):
        group, s = self.fetched
        loaded, sums, w = self.loaded, self.sums, group.width
        many, at, terms, stride = ((4, 1, 2, 4), (2, 3, 3, 1), (1, 0, 4, 1), (1, 0, 5, 1))[s]
        base = (0, 4, 6, 0)[s]
        before = self.last.get(s)

        def one(t):
            for c in self.loads(group, s, t):
                c.wait()
            if s < 3 and before is not None:
                self.message(before, t.p, s + 2).wait_send()

            step = 512

            def unit(u, _):
                i, cols = u // (w // step), pl.ds(pl.multiple_of(u % (w // step) * step, step), step)
                total = sum(loaded[t.p, i * at + m * stride, :, cols].astype(F32) for m in range(terms)).astype(BF)
                if s < 3:
                    sums[t.p, base + i, :, cols] = total
                else:
                    group.out_ref[group.layer, group.rows(t.p), pl.ds(pl.multiple_of(group.first + u * step, step), step)] = total
                    sq = total.astype(F32)
                    sq = (sq * sq).reshape(-1, *self.ss.shape[:1], step).sum(0)
                    self.ss[...] += sum(sq[:, m : m + 128] for m in range(0, step, 128))
                return 0

            lax.fori_loop(0, many * (w // step), unit, 0)
            if s < 3:
                to = (t.device(t.c2, t.e), t.device(t.c, t.e1), t.device(t.c, t.e2))[s]
                src = sums.at[t.p, pl.ds(base, HELD[s + 2][1]), :, pl.ds(0, w)]
                self.remote(src, group.got(t.p, *HELD[s + 2]), group.index, t.p, s + 2, to).start()

        self.parts(one)
        self.last[s] = group
        if s == 0:
            self.started.append(group)

    def finish(self):
        def one(t):
            for group in self.started:
                for k in (0, 1):
                    self.message(group, t.p, k).wait_send()
            for s in range(3):
                self.message(self.last[s], t.p, s + 2).wait_send()

        self.parts(one)

    def total(self, out, got, send_sem, recv_sem):
        src = self.ss
        for k, (place, line) in enumerate(zip((self.x, self.y), self.lines())):
            got[k, place] = src[...]
            copies = [
                pltpu.make_async_remote_copy(
                    src_ref=src, dst_ref=got.at[k, place], send_sem=send_sem.at[k, d], recv_sem=recv_sem.at[k, d],
                    device_id={self.axis: peer}, device_id_type=pl.DeviceIdType.MESH,
                )
                for d, peer in enumerate(line)
            ]
            for c in copies:
                c.start()
            for c in copies:
                c.wait()
            out[...] = sum(got[k, i] for i in range(self.side))
            src = out


def reduce_scratch(high, wide, groups, side):
    dma = pltpu.SemaphoreType.DMA
    vec = (8, 128)
    return [
        pltpu.VMEM((PARTS, 8, high, wide), BF), pltpu.VMEM((PARTS, 7, high, wide), BF), pltpu.VMEM(vec, F32),
        dma((PARTS, 8)), dma((groups, PARTS, 5)), dma((groups, PARTS, 5)),
        pltpu.VMEM(vec, F32), pltpu.VMEM((2, side, *vec), F32), dma((2, side)), dma((2, side)),
    ]


def pipeline(n, loads, work, stores, ready=(), after=None, every=1, hooks=None):
    for c in loads(0, 0):
        c.start()
    for f in ready:
        f()

    def written(j):
        for c in stores(j, j % 2):
            c.wait()

    def tile(j, _):
        slot = j % 2

        @pl.when(j + 1 < n)
        def _():
            for c in loads(j + 1, 1 - slot):
                c.start()

        for c in loads(j, slot):
            c.wait()
        work(j, slot)
        for c in stores(j, slot):
            c.start()

        @pl.when(j > 0)
        def _():
            written(j - 1)

        if after is not None:

            @pl.when((j > 0) & (j % every == 0))
            def _():
                after(j - every)

        for at, todo in (hooks or {}).items():

            @pl.when(j == at)
            def _(todo=todo):
                for f in todo:
                    f()

        return 0

    lax.fori_loop(0, n, tile, 0)
    written(n - 1)
    if after is not None:
        after(n - every)


def backward(dy, dyt, wg, wu, wd, h1, a0t, a1t, z, by_gate, by_up, ms, vs, axis, n):
    T, D = dy.shape
    FF = z.shape[2]
    db, fb, side, L = D // n, FF // n, round(n**0.5), wg.shape[0]
    H = 2 * db
    high, wide = H // PARTS, D // H * fb
    cuts = [[FF // 8 * k for k in ks] for ks in ((0, 3, 6, 8), (0, 4, 8))]
    bd, bg, bt = 2 * fb, 256, 256
    k = bd // fb
    n_groups = L + sum(len(c) - 1 for c in cuts)
    piece, lane = 512, 128
    q, r = db // PARTS, fb // PARTS
    h = L * q
    count = n * sum(m.size for m in ms)

    def body(*refs):
        (dy_h, dyt_h, wg_h, wu_h, wd_h, h1_h, a0t_h, a1t_h, z_h, p_h, q_h), moments_h, refs = refs[:11], refs[11:17], refs[17:]
        new_h, refs = refs[:PARTS], refs[PARTS:]
        (d_out, gu_out, ss_out, d_got, gu_got, d_own, gu_own, dg_h, du_h), (d_sum, gu_sum), refs = refs[:9], refs[9:11], refs[11:]
        red = Reducer(axis, side, *refs[:-4])
        copy = pltpu.make_async_copy
        index = iter(range(n_groups))
        down_of = [Group(next(index), l, d_own, d_got, d_sum, 0, wide) for l in range(L)]
        gate_of = [[Group(next(index), l, gu_own, gu_got, gu_sum, a, b - a) for a, b in zip(cuts[l], cuts[l][1:])] for l in range(L)]

        named = dict(zip("dDabcAB", down_of + gate_of[0] + gate_of[1]))
        left = {name: iter(range(4)) for name in named}

        def fetch(name):
            red.fetch(named[name], next(left[name]))

        def steps(plan):
            hooks = {}
            for t, name in enumerate(plan):
                if t and plan[t - 1] != ".":
                    hooks[t] = [red.add]
                if name != ".":
                    hooks.setdefault(t, []).append(functools.partial(fetch, name))
            return hooks

        def down_grad(dyt_v, l, plan, ready):
            def scope(z_v, o_v, zs, os):
                def loads(j, slot):
                    return [copy(z_h.at[l, :, pl.ds(pl.multiple_of(j * bd, bd), bd)], z_v.at[slot], zs.at[slot])]

                def stores(j, slot):
                    a, b = j * k // side, j * k % side
                    return [copy(o_v.at[slot], d_own.at[l, a, pl.ds(b, k)], os.at[slot])]

                def work(j, slot):
                    for i in range(D // piece):
                        g = mm(dyt_v[pl.ds(i * piece, piece), :], z_v[slot]).astype(BF)
                        for r in range(piece // H):
                            to = (i * (piece // H) + r) * fb
                            for c in range(k):
                                o_v[slot, c, :, to : to + fb] = g[r * H : (r + 1) * H, c * fb : (c + 1) * fb]

                def after(j):
                    red.send_row(down_of[l], j * k // side)

                pipeline(FF // bd, loads, work, stores, ready, after, side // k, steps(plan))

            two = pltpu.SemaphoreType.DMA((2,))
            pl.run_scoped(scope, pltpu.VMEM((2, T, bd), BF), pltpu.VMEM((2, k, H, wide), BF), two, two)

        def gate_up_grad(dy_v, at_v, l, keep, every, plan, ready):
            def scope(w_t, p_v, q_v, dg_v, du_v, o_v, ins, os):
                def tile(j):
                    return pl.ds(pl.multiple_of(j * bg, bg), bg)

                def loads(j, slot):
                    pairs = ((wd_h.at[l, tile(j), :], w_t), (p_h.at[l, :, tile(j)], p_v), (q_h.at[l, :, tile(j)], q_v))
                    return [copy(src, dst.at[slot], ins.at[slot, i]) for i, (src, dst) in enumerate(pairs)]

                def stores(j, slot):
                    out = [copy(o_v.at[slot], gu_own.at[l, :, :, :, tile(j)], os.at[slot, 0])]
                    if keep:
                        out.append(copy(dg_v.at[slot], dg_h.at[:, tile(j)], os.at[slot, 1]))
                        out.append(copy(du_v.at[slot], du_h.at[:, tile(j)], os.at[slot, 2]))
                    return out

                def work(j, slot):
                    for i in range(0, T, piece):
                        at = pl.ds(i, piece)
                        dz = mm_nt(dy_v[at, :], w_t[slot]).astype(BF).astype(F32)
                        dg_v[slot, at, :] = (dz * p_v[slot, at, :]).astype(BF)
                        du_v[slot, at, :] = (dz * q_v[slot, at, :]).astype(BF)
                    for i in range(0, D, piece):
                        at = pl.ds(i, piece)
                        for half, d_v in enumerate((dg_v, du_v)):
                            g = mm(at_v[at, :], d_v[slot]).astype(BF)
                            for b in range(piece // db):
                                block = i // db + b
                                o_v[slot, block // side, block % side, half * db : (half + 1) * db, :] = g[b * db : (b + 1) * db]

                def after(j):
                    red.send_columns(l, gu_own, gu_got, gate_of[l], j * bg, every * bg)

                pipeline(FF // bg, loads, work, stores, ready, after, every, steps(plan))

            six = pltpu.SemaphoreType.DMA((2, 3))
            f, b = pltpu.VMEM((2, T, bg), F32), pltpu.VMEM((2, T, bg), BF)
            pl.run_scoped(scope, pltpu.VMEM((2, bg, D), BF), f, f, b, b, pltpu.VMEM((2, side, side, H, bg), BF), six, six)

        def norm_grad(dy_v, dyt_v, w_v, plan, ready):
            def scope(dg_v, du_v, h_v, da_0, da_1, ins):
                def tile(j):
                    return pl.ds(pl.multiple_of(j * bt, bt), bt)

                def rows_before(j):
                    return tile(jnp.maximum(j - 1, 0))

                def loads(j, slot):
                    pairs = ((dg_h.at[tile(j), :], dg_v), (du_h.at[tile(j), :], du_v), (h1_h.at[rows_before(j), :], h_v))
                    return [copy(src, dst.at[slot], ins.at[slot, i]) for i, (src, dst) in enumerate(pairs)]

                def one(j, slot, da_v, before_v):
                    at = rows_before(j)
                    old = dy_v[at, :]
                    new = old + norm_back(h_v[slot], before_v[...].astype(F32), D)
                    new = jnp.where(j > 0, new, old)
                    da_v[...] = mm_nt(dg_v[slot], w_v[0]).astype(BF) + mm_nt(du_v[slot], w_v[1]).astype(BF)
                    dy_v[at, :] = new
                    dyt_v[:, at] = new.T

                def work(j, slot):
                    for s, pair in enumerate(((da_0, da_1), (da_1, da_0))):
                        pl.when(slot == s)(functools.partial(one, j, s, *pair))

                pipeline(T // bt, loads, work, lambda j, slot: [], ready, hooks=steps(plan))
                last = T // bt
                get_h = copy(h1_h.at[rows_before(last), :], h_v.at[last % 2], ins.at[last % 2, 2])
                get_h.start()
                get_h.wait()
                at = rows_before(last)
                new = dy_v[at, :] + norm_back(h_v[last % 2], (da_1 if last % 2 == 0 else da_0)[...].astype(F32), D)
                dy_v[at, :] = new
                dyt_v[:, at] = new.T

            wide_t, da = pltpu.VMEM((2, bt, FF), BF), pltpu.VMEM((bt, D), BF)
            pl.run_scoped(scope, wide_t, wide_t, pltpu.VMEM((2, bt, D), BF), da, da, pltpu.SemaphoreType.DMA((2, 3)))

        def layers(dy_v, dyt_v, at_v, w_v, sem):
            pairs = ((dyt_h, dyt_v), (dy_h, dy_v), (a1t_h, at_v), (wg_h.at[1], w_v.at[0]), (wu_h.at[1], w_v.at[1]), (a0t_h, at_v))
            get_dyt, *others, get_at0 = [copy(src, dst, sem.at[i]) for i, (src, dst) in enumerate(pairs)]
            get_dy, get_at, get_wg, get_wu = others
            get_dyt.start()
            red.ss[...] = jnp.zeros_like(red.ss)
            down_grad(dyt_v, 1, "", [red.greet, get_dyt.wait] + [c.start for c in others])
            gate_up_grad(dy_v, at_v, 1, True, 4, "..D.....D.....A.", (get_dy.wait, get_at.wait))
            get_at0.start()
            norm_grad(dy_v, dyt_v, w_v, "..ADBA..", (get_wg.wait, get_wu.wait))
            down_grad(dyt_v, 0, "B.......", ())
            gate_up_grad(dy_v, at_v, 0, False, 2, "B.d......d......", (get_at0.wait,))

        t_d, d_t = pltpu.VMEM((T, D), BF), pltpu.VMEM((D, T), BF)
        pl.run_scoped(layers, t_d, d_t, d_t, pltpu.VMEM((2, D, FF), BF), pltpu.SemaphoreType.DMA((6,)))

        def rest(mg, mu, md, vg, vu, vd, w_g, w_u, w_d, g_v, new_v, sem, new_sem, sum_sem):
            me = lax.axis_index(axis)
            mine = pl.ds(pl.multiple_of(me * db, db), db)
            srcs = moments_h + (wg_h.at[:, mine], wu_h.at[:, mine], wd_h.at[:, pl.ds(pl.multiple_of(me * fb, fb), fb)])
            gets = [copy(src, dst, sem.at[i]) for i, (src, dst) in enumerate(zip(srcs, (mg, mu, md, vg, vu, vd, w_g, w_u, w_d)))]
            for c in gets:
                c.start()
            for name in "aBDAdbcabcdabcabc":
                fetch(name)
                red.add()
            red.finish()
            puts = [copy(d_sum, d_out, sum_sem.at[0]), copy(gu_sum, gu_out, sum_sem.at[1])]
            for c in puts:
                c.start()
            for c in gets:
                c.wait()
            out, *others = refs[-4:]
            red.total(out, *others)
            ss_out[...] = out[...]
            factor = clip_factor(jnp.sum(jnp.sum(out[...], 0, keepdims=True), 1, keepdims=True), count)

            def part(p, _):
                for i, (w, m, v) in enumerate(((w_g, mg, vg), (w_u, mu, vu))):
                    for l in range(L):
                        here, from_ = pl.ds(pl.multiple_of(p * q, q), q), pl.ds(pl.multiple_of(i * db + p * q, q), q)
                        to = pl.ds(i * h + l * q, q)

                        def some(t, _):
                            at = l, here, pl.ds(pl.multiple_of(t * D, D), D)
                            new_v[p, to, at[2]] = adamw(w[at].astype(F32), m[at], v[at], gu_sum[l, from_, at[2]].astype(F32) * factor)
                            return 0

                        lax.fori_loop(0, FF // D, some, 0)
                first, skip = pl.multiple_of(p * r // lane * lane, lane), pl.multiple_of(p * r % lane, r)
                here = pl.ds(pl.multiple_of(p * r, r), r)
                for l in range(L):
                    for t in range(D // H):
                        g_v[:, t * H : (t + 1) * H] = d_sum[l, :, pl.ds(t * fb + first, lane)].astype(F32).T
                    new = adamw(w_d[l, here, :].astype(F32), md[l, here, :], vd[l, here, :], g_v[pl.ds(skip, r), :] * factor)
                    for s in range(0, r, h):
                        c = (l * r + s) // h
                        new_v[p, 2 * h :, c * D : (c + 1) * D] = new[s : s + h]
                for i, new in enumerate(new_h):
                    pl.when(p == i)(copy(new_v.at[i], new, new_sem.at[i]).start)
                return 0

            lax.fori_loop(0, PARTS, part, 0)
            for i, new in enumerate(new_h):
                copy(new_v.at[i], new, new_sem.at[i]).wait()
            for c in puts:
                c.wait()

        dma = pltpu.SemaphoreType.DMA
        moments = [pltpu.VMEM(m.shape, F32) for m in ms]
        pl.run_scoped(
            rest, *moments, *moments, *[pltpu.VMEM(m.shape, BF) for m in ms], pltpu.VMEM((lane, D), F32), pltpu.VMEM((PARTS, 3 * h, FF), BF),
            dma((9,)), dma((PARTS,)), dma((2,)),
        )

    anys = pl.BlockSpec(memory_space=pl.ANY)
    shape = jax.ShapeDtypeStruct
    outs = pl.pallas_call(
        body,
        in_specs=[anys] * 17,
        out_specs=[anys] * (PARTS + 2) + [pl.BlockSpec(memory_space=pltpu.VMEM)] + [anys] * 6,
        out_shape=[
            *[shape((3 * h, FF), BF)] * PARTS, shape((L, H, wide), BF), shape((L, H, FF), BF), shape((8, 128), F32),
            shape((L, PARTS, SLOTS, high, wide), BF), shape((L, PARTS, SLOTS, high, FF), BF),
            shape((L, side, side, H, wide), BF), shape((L, side, side, H, FF), BF), shape((T, FF), BF), shape((T, FF), BF),
        ],
        scratch_shapes=[pltpu.VMEM((L, H, wide), BF), pltpu.VMEM((L, H, FF), BF), *reduce_scratch(high, wide, n_groups, side)],
        compiler_params=pltpu.CompilerParams(collective_id=0, has_side_effects=True, vmem_limit_bytes=67043328),
        cost_estimate=cost(18 * T * D * FF, 10**9),
        name="backward",
    )(dy, dyt, wg, wu, wd, h1, a0t, a1t, z, by_gate, by_up, *ms, *vs)
    return outs[:PARTS], *outs[PARTS : PARTS + 3]


def solution(mesh):
    axis = "dp"
    n = mesh.shape[axis]

    def step(x, dy, wg, wu, wd, mg, mu, md, vg, vu, vd):
        x, dy = x[0], dy[0]
        z, p, q, h1, a0t, a1t, dyt = forward(x, dy, wg, wu, wd)
        ms, vs = (mg, mu, md), (vg, vu, vd)
        packed, gd, gu, squares = backward(dy, dyt, wg, wu, wd, h1, a0t, a1t, z, p, q, ms, vs, axis, n)
        count = n * sum(m.size for m in ms)

        def moments(gd, gu, squares):
            factor = clip_factor(jnp.sum(squares), count)
            (L, db), fb = mg.shape[:2], md.shape[1]
            by_down = gd.reshape(*gd.shape[:2], -1, fb).transpose(0, 3, 2, 1).reshape(md.shape)
            new = [new_moments(m, v, g.astype(F32) * factor) for m, v, g in zip(ms, vs, (gu[:, :db], gu[:, db:], by_down))]
            return [t[0] for t in new] + [t[1] for t in new]

        whole, done = gather(packed, mg.shape, md.shape, axis, n, (gd, gu, squares), moments)
        return (*whole, *done)

    seq, all_, rows = P(("rep", axis)), P(), P(None, axis)
    return jax.shard_map(
        step,
        mesh=mesh,
        in_specs=(seq, seq, *[all_] * 3, *[rows] * 6),
        out_specs=(*[P("rep")] * 3, *[P("rep", axis)] * 6),
        check_vma=False,
    )
```
